8 devices in a mesh: dp: 1 (over z), tp: 8 (over y, x, core).
Axes of the slice: x: 2, y: 2, z: 1, core: 2. Of those that a mesh axis runs over, the one named last changes fastest.
Arguments:
- x_in: bfloat16 [8, 2048, 2560], P('dp', 'tp')
- ln_gain: float32 [2, 2560], replicated
- ln_bias: float32 [2, 2560], replicated
- w_qkv: bfloat16 [2, 2560, 3, 32, 80], P(None, None, None, 'tp')
- w_out: bfloat16 [2, 32, 80, 2560], P(None, 'tp')
- b_out: float32 [2, 2560], replicated
- w_up: bfloat16 [2, 2560, 10240], P(None, None, 'tp')
- b_up: float32 [2, 10240], P(None, 'tp')
- w_down: bfloat16 [2, 10240, 2560], P(None, 'tp')
- b_down: float32 [2, 2560], replicated
Outputs:
- output: bfloat16 [8, 2048, 2560], P('dp', 'tp')
All inputs are finite; a program needn't handle non-finite values.
Results may differ from the reference program's by a relative error of at most 0.0128346.
Values are sent between devices in bfloat16 or wider.
A program may use at most 1 GiB of HBM per device.

```python
import math
import jax
import jax.numpy as jnp
from jax import lax

BATCH_SIZE = 8
SEQ_LEN = 2048
MODEL_DIM = 2560
N_HEADS = 32
HEAD_DIM = 80
FFN_WIDTH = 10240
NUM_LAYERS = 2
LN_EPS = 1e-5


def setup_inputs(seed: int = 0, part: int = 0) -> dict:
    key = jax.random.key(seed)
    shared = jax.random.split(key, 9)
    part_keys = jax.random.split(jax.random.fold_in(key, part), 2)
    tok_scale = 0.5 + jax.random.uniform(part_keys[0], (BATCH_SIZE, SEQ_LEN, 1), jnp.float32)
    x_in = jax.random.normal(part_keys[1], (BATCH_SIZE, SEQ_LEN, MODEL_DIM), jnp.float32) * tok_scale
    logit_std = math.sqrt(max(math.log(SEQ_LEN / 32.0), 1.0))
    qk_gain = math.sqrt(logit_std)
    comp_gain = jnp.array([qk_gain, qk_gain, 1.0], jnp.float32).reshape(1, 1, 3, 1, 1)
    in_scale = MODEL_DIM ** -0.5
    w_qkv = jax.random.normal(shared[0], (NUM_LAYERS, MODEL_DIM, 3, N_HEADS, HEAD_DIM), jnp.float32) * (in_scale * comp_gain)
    w_out = jax.random.normal(shared[1], (NUM_LAYERS, N_HEADS, HEAD_DIM, MODEL_DIM), jnp.float32) * (1.5 * in_scale)
    w_up = jax.random.normal(shared[2], (NUM_LAYERS, MODEL_DIM, FFN_WIDTH), jnp.float32) * in_scale
    w_down = jax.random.normal(shared[3], (NUM_LAYERS, FFN_WIDTH, MODEL_DIM), jnp.float32) * FFN_WIDTH ** -0.5
    ln_gain = 1.0 + 0.2 * jax.random.normal(shared[4], (NUM_LAYERS, MODEL_DIM), jnp.float32)
    ln_bias = 0.2 * jax.random.normal(shared[5], (NUM_LAYERS, MODEL_DIM), jnp.float32)
    b_out = 0.1 * jax.random.normal(shared[6], (NUM_LAYERS, MODEL_DIM), jnp.float32)
    b_up = 0.3 * jax.random.normal(shared[7], (NUM_LAYERS, FFN_WIDTH), jnp.float32)
    b_down = 0.1 * jax.random.normal(shared[8], (NUM_LAYERS, MODEL_DIM), jnp.float32)
    return {
        'x_in': x_in.astype(jnp.bfloat16),
        'ln_gain': ln_gain,
        'ln_bias': ln_bias,
        'w_qkv': w_qkv.astype(jnp.bfloat16),
        'w_out': w_out.astype(jnp.bfloat16),
        'b_out': b_out,
        'w_up': w_up.astype(jnp.bfloat16),
        'b_up': b_up,
        'w_down': w_down.astype(jnp.bfloat16),
        'b_down': b_down,
    }


def layer_norm(residual, gain, bias):
    row_mean = jnp.mean(residual, axis=-1, keepdims=True)
    centered = residual - row_mean
    row_var = jnp.mean(centered * centered, axis=-1, keepdims=True)
    return (centered * lax.rsqrt(row_var + LN_EPS) * gain + bias).astype(jnp.bfloat16)


def query_block(batch, heads, q_len, k_len):
    block = q_len
    while block % 2 == 0 and block > 16 and batch * heads * block * k_len > 2 ** 24:
        block = block // 2
    return block


def causal_attention(queries, keys, values):
    batch, seq_len, heads, head_dim = queries.shape
    block = query_block(batch, heads, seq_len, seq_len)
    inv_sqrt = head_dim ** -0.5
    key_pos = jnp.arange(seq_len)
    keys_f = keys.astype(jnp.float32)
    values_f = values.astype(jnp.float32)

    def one_block(index):
        q_blk = lax.dynamic_slice_in_dim(queries, index * block, block, axis=1).astype(jnp.float32)
        scores = jnp.einsum('bqhe,bkhe->bhqk', q_blk, keys_f) * inv_sqrt
        q_pos = index * block + jnp.arange(block)
        scores = jnp.where(key_pos[None, :] <= q_pos[:, None], scores, -jnp.inf)
        attn_prob = jax.nn.softmax(scores, axis=-1).astype(jnp.bfloat16).astype(jnp.float32)
        return jnp.einsum('bhqk,bkhe->bqhe', attn_prob, values_f).astype(jnp.bfloat16)

    out_blocks = lax.map(one_block, jnp.arange(seq_len // block))
    return jnp.moveaxis(out_blocks, 0, 1).reshape(batch, seq_len, heads, head_dim)


def one_layer(residual, params):
    ln_gain, ln_bias, w_qkv, w_out, b_out, w_up, b_up, w_down, b_down = params
    normed = layer_norm(residual, ln_gain, ln_bias)
    normed_f = normed.astype(jnp.float32)
    qkv_all = jnp.einsum('bsd,dthe->bsthe', normed_f, w_qkv.astype(jnp.float32)).astype(jnp.bfloat16)
    attn_out = causal_attention(qkv_all[:, :, 0], qkv_all[:, :, 1], qkv_all[:, :, 2])
    attn_sum = jnp.einsum('bshe,hed->bsd', attn_out.astype(jnp.float32), w_out.astype(jnp.float32))
    hidden = jnp.einsum('bsd,df->bsf', normed_f, w_up.astype(jnp.float32)) + b_up
    gelu_out = jax.nn.gelu(hidden, approximate=True).astype(jnp.bfloat16)
    mlp_sum = jnp.einsum('bsf,fd->bsd', gelu_out.astype(jnp.float32), w_down.astype(jnp.float32))
    return residual + (attn_sum + mlp_sum + b_out + b_down), None


def reference(x_in, ln_gain, ln_bias, w_qkv, w_out, b_out, w_up, b_up, w_down, b_down):
    residual = x_in.astype(jnp.float32)
    residual, _ = lax.scan(one_layer, residual, (ln_gain, ln_bias, w_qkv, w_out, b_out, w_up, b_up, w_down, b_down))
    return residual.astype(jnp.bfloat16)
```

```python
import functools

import jax
import jax.numpy as jnp
from jax import lax
from jax.experimental import pallas as pl
from jax.experimental.pallas import tpu as pltpu
from jax.sharding import PartitionSpec as P


LN_EPS = 1e-5
LOG2_E = 1.4426950408889634
BLK = 256
SHARDS = 4
VMEM_LIMIT = 62 * 2 ** 20


def attn_kernel(pos_ref, *refs, heads, dim):
    own, oth = refs[:SHARDS], refs[SHARDS:2 * SHARDS]
    o_own, o_oth, q_s, k_s, v_s, o_s, s_a, s_b, p_a, p_b = refs[2 * SHARDS:]
    tokens = o_s.shape[1]
    per_half = o_own.shape[0] // BLK
    for half, group in enumerate((own, oth)):
        for rel in range(per_half):
            off = pl.multiple_of(pos_ref[half * per_half + rel], BLK)
            cols = slice(rel * BLK, (rel + 1) * BLK)
            for shard, ref in enumerate(group):
                def stage(h, _, ref=ref, shard=shard, cols=cols, off=off):
                    def rows(t):
                        return pl.ds(pl.multiple_of((t * heads + h) * dim, 16), dim)

                    head = shard * heads + h
                    q_s[head, :, pl.ds(off, BLK)] = ref[rows(0), cols]
                    k_s[head, pl.ds(off, BLK), :dim] = ref[rows(1), cols].T
                    v_s[head, :, pl.ds(off, BLK)] = ref[rows(2), cols]
                    return 0

                lax.fori_loop(0, heads, stage, 0, unroll=True)

    scale = dim ** -0.5 * LOG2_E
    n_q = tokens // BLK
    s_bufs, p_bufs = (s_a, s_b), (p_a, p_b)

    def one_head(head, _):
        keep = (lax.broadcasted_iota(jnp.int32, (BLK, BLK), 0)
                <= lax.broadcasted_iota(jnp.int32, (BLK, BLK), 1))

        def scores(qi):
            end = (qi + 1) * BLK
            s_ref = s_bufs[qi % 2]
            s = jnp.dot(k_s[head, :end, :dim], q_s[head, :, qi * BLK:end], preferred_element_type=jnp.float32)
            if qi:
                s_ref[:end - BLK, :] = s[:end - BLK]
            s_ref[end - BLK:end, :] = jnp.where(keep, s[end - BLK:], -jnp.inf)

        def soften(qi):
            s_ref, p_ref = s_bufs[qi % 2], p_bufs[qi % 2]
            top = None
            for ki in range(qi + 1):
                cur = s_ref[ki * BLK:(ki + 1) * BLK, :].reshape(BLK // 8, 8, BLK).max(axis=0)
                top = cur if top is None else jnp.maximum(top, cur)
            top = top.max(axis=0, keepdims=True) * scale
            total = None
            for ki in range(qi + 1):
                p = jnp.exp2(s_ref[ki * BLK:(ki + 1) * BLK, :] * scale - top)
                part = p.reshape(BLK // 8, 8, BLK).sum(axis=0)
                total = part if total is None else total + part
                p_ref[ki * BLK:(ki + 1) * BLK, :] = p.astype(jnp.bfloat16)
            return total.sum(axis=0, keepdims=True)

        def weigh(qi, total):
            end = (qi + 1) * BLK
            acc = jnp.dot(v_s[head, :, :end], p_bufs[qi % 2][:end, :], preferred_element_type=jnp.float32)
            rows = pl.ds(pl.multiple_of(head * dim, 16), dim)
            o_s[rows, qi * BLK:end] = (acc / total).astype(jnp.bfloat16)

        scores(0)
        previous = None
        for qi in range(n_q):
            if qi + 1 < n_q:
                scores(qi + 1)
            total = soften(qi)
            if previous is not None:
                weigh(qi - 1, previous)
            previous = total
        weigh(n_q - 1, previous)
        return 0

    lax.fori_loop(0, SHARDS * heads, one_head, 0)
    for half, out in enumerate((o_own, o_oth)):
        for rel in range(per_half):
            off = pl.multiple_of(pos_ref[half * per_half + rel], BLK)
            out[rel * BLK:(rel + 1) * BLK, :] = o_s[:, pl.ds(off, BLK)].T


def attention(pos, own, oth, heads, dim):
    half_tokens = own[0].shape[1]
    tokens, all_heads = 2 * half_tokens, SHARDS * heads
    shape = jax.ShapeDtypeStruct((half_tokens, all_heads * dim), jnp.bfloat16)
    vmem = pl.BlockSpec(memory_space=pltpu.VMEM)
    return pl.pallas_call(
        functools.partial(attn_kernel, heads=heads, dim=dim),
        out_shape=(shape, shape),
        in_specs=[pl.BlockSpec(memory_space=pltpu.SMEM)] + [vmem] * (2 * SHARDS),
        out_specs=(vmem, vmem),
        scratch_shapes=[
            pltpu.VMEM((all_heads, dim, tokens), jnp.bfloat16),
            pltpu.VMEM((all_heads, tokens, 128), jnp.bfloat16),
            pltpu.VMEM((all_heads, dim, tokens), jnp.bfloat16),
            pltpu.VMEM((all_heads * dim, tokens), jnp.bfloat16),
            pltpu.VMEM((tokens, BLK), jnp.float32),
            pltpu.VMEM((tokens, BLK), jnp.float32),
            pltpu.VMEM((tokens, BLK), jnp.bfloat16),
            pltpu.VMEM((tokens, BLK), jnp.bfloat16),
        ],
        compiler_params=pltpu.CompilerParams(vmem_limit_bytes=VMEM_LIMIT),
        cost_estimate=pl.CostEstimate(
            flops=5 * all_heads * tokens * tokens * dim, bytes_accessed=4 * 2 * tokens * all_heads * dim,
            transcendentals=all_heads * tokens * tokens // 2),
    )(pos, *own, *oth)


def combine_kernel(*refs, first):
    n = (len(refs) - 3) // 2
    lhs_hbm, rhs, (out, lhs, sems) = refs[:n], refs[n:2 * n], refs[2 * n:]
    rows = out.shape[0]
    step = 512
    copies = [pltpu.make_async_copy(lhs_hbm[i].at[pl.ds(first, rows)], lhs.at[i], sems.at[i]) for i in range(n)]

    @pl.when(pl.program_id(0) == 0)
    def _():
        for copy in copies:
            copy.start()

    def product(wait):
        for r in range(0, rows, step):
            acc = None
            for i in range(n):
                if wait and r == 0:
                    copies[i].wait()
                term = jnp.dot(lhs[i, r:r + step, :], rhs[i][...], preferred_element_type=jnp.float32)
                acc = term if acc is None else acc + term
            out[r:r + step, :] = acc.astype(out.dtype)

    @pl.when(pl.program_id(0) == 0)
    def _():
        product(True)

    @pl.when(pl.program_id(0) > 0)
    def _():
        product(False)


def combine(lhs, rhs, dtype, first=0, rows=None):
    rows = rows or lhs[0].shape[0]
    depth = lhs[0].shape[1]
    width = rhs[0].shape[1]
    tile = 256
    return pl.pallas_call(
        functools.partial(combine_kernel, first=first),
        out_shape=jax.ShapeDtypeStruct((rows, width), dtype),
        grid=(width // tile,),
        in_specs=[pl.BlockSpec(memory_space=pl.ANY) for _ in lhs]
        + [pl.BlockSpec((depth, tile), lambda n: (0, n)) for _ in rhs],
        out_specs=pl.BlockSpec((rows, tile), lambda n: (0, n)),
        scratch_shapes=[pltpu.VMEM((len(lhs), rows, depth), jnp.bfloat16), pltpu.SemaphoreType.DMA((len(lhs),))],
        compiler_params=pltpu.CompilerParams(vmem_limit_bytes=VMEM_LIMIT, dimension_semantics=("arbitrary",)),
        cost_estimate=pl.CostEstimate(
            flops=2 * rows * depth * len(lhs) * width, bytes_accessed=2 * depth * len(lhs) * (rows + width) + 4 * rows * width,
            transcendentals=0),
    )(*lhs, *rhs)


def qkv_kernel(h_ref, w_a, w_b, out_a, out_b):
    step = pl.program_id(0)
    last = pl.num_programs(0) // 2

    def project(w_ref, out):
        h = h_ref[...]
        prod = lax.dot_general(w_ref[...], h, (((1,), (1,)), ((), ())), preferred_element_type=jnp.float32)
        out[...] = prod.astype(jnp.bfloat16)

    @pl.when(step < last)
    def _():
        project(w_a, out_a)

    @pl.when(step >= last)
    def _():
        project(w_b, out_b)


def qkv_pair(h, w_a, w_b):
    tokens, width = h.shape
    rows = w_a.shape[0]
    tile = rows // 2
    shape = jax.ShapeDtypeStruct((rows, tokens), jnp.bfloat16)
    early = lambda n: (jnp.minimum(n, 1), 0)
    late = lambda n: (jnp.maximum(n - 2, 0), 0)
    return pl.pallas_call(
        qkv_kernel,
        out_shape=(shape, shape),
        grid=(4,),
        in_specs=[pl.BlockSpec((tokens, width), lambda n: (0, 0), pipeline_mode=pl.Buffered(1)),
                  pl.BlockSpec((tile, width), early), pl.BlockSpec((tile, width), late)],
        out_specs=(pl.BlockSpec((tile, tokens), early), pl.BlockSpec((tile, tokens), late)),
        compiler_params=pltpu.CompilerParams(vmem_limit_bytes=VMEM_LIMIT, dimension_semantics=("arbitrary",)),
        cost_estimate=pl.CostEstimate(flops=4 * tokens * width * rows, bytes_accessed=2 * (tokens * width + 2 * rows * (width + tokens)),
                                      transcendentals=0),
    )(h, w_a, w_b)


def up_kernel(h_ref, *refs):
    n = len(refs) // 3
    weights, biases, outs = refs[:n], refs[n:2 * n], refs[2 * n:]
    per_shard = pl.num_programs(0) // n
    rows = h_ref.shape[0]
    for i in range(n):
        @pl.when(pl.program_id(0) // per_shard == i)
        def _(i=i):
            for r in range(0, rows, 512):
                hidden = jnp.dot(h_ref[r:r + 512, :], weights[i][...], preferred_element_type=jnp.float32) + biases[i][...]
                outs[i][r:r + 512, :] = jax.nn.gelu(hidden, approximate=True).astype(jnp.bfloat16)


def up(h, weights, biases):
    tokens, width = h.shape
    n, cols = len(weights), weights[0].shape[1]
    tile = 256
    per_shard = cols // tile
    at = [lambda s, i=i: (0, jnp.clip(s - i * per_shard, 0, per_shard - 1)) for i in range(n)]
    return pl.pallas_call(
        up_kernel,
        out_shape=[jax.ShapeDtypeStruct((tokens, cols), jnp.bfloat16)] * n,
        grid=(n * per_shard,),
        in_specs=[pl.BlockSpec((tokens, width), lambda s: (0, 0), pipeline_mode=pl.Buffered(1))]
        + [pl.BlockSpec((width, tile), m) for m in at] + [pl.BlockSpec((1, tile), m) for m in at],
        out_specs=[pl.BlockSpec((tokens, tile), m) for m in at],
        compiler_params=pltpu.CompilerParams(vmem_limit_bytes=VMEM_LIMIT, dimension_semantics=("arbitrary",)),
        cost_estimate=pl.CostEstimate(flops=2 * n * tokens * width * cols,
                                      bytes_accessed=2 * (tokens * width + n * cols * (width + tokens)),
                                      transcendentals=n * tokens * cols),
    )(h, *weights, *[b.reshape(1, cols) for b in biases])


def norm_block(res, gain, bias):
    mean = jnp.mean(res, axis=-1, keepdims=True)
    centered = res - mean
    var = jnp.mean(centered * centered, axis=-1, keepdims=True)
    return (centered * lax.rsqrt(var + LN_EPS) * gain + bias).astype(jnp.bfloat16)


def update_kernel(res, kept, received, bias_sum, gain, bias, res_out, h_out):
    new = res[...].astype(jnp.float32) + (kept[...] + received[...].astype(jnp.float32) + bias_sum[...])
    res_out[...] = new
    h_out[...] = norm_block(new, gain[...], bias[...])


def update_norm(res, kept, received, bias_sum, gain, bias):
    tokens, width = res.shape
    tile = 128
    row = pl.BlockSpec((tile, width), lambda n: (n, 0))
    vec = pl.BlockSpec((1, width), lambda n: (0, 0))
    return pl.pallas_call(
        update_kernel,
        out_shape=(jax.ShapeDtypeStruct((tokens, width), jnp.float32), jax.ShapeDtypeStruct((tokens, width), jnp.bfloat16)),
        grid=(tokens // tile,),
        in_specs=[row, row, row, vec, vec, vec],
        out_specs=(row, row),
        compiler_params=pltpu.CompilerParams(vmem_limit_bytes=VMEM_LIMIT, dimension_semantics=("arbitrary",)),
        cost_estimate=pl.CostEstimate(flops=10 * tokens * width, bytes_accessed=16 * tokens * width, transcendentals=0),
    )(res, kept, received, bias_sum.reshape(1, width), gain.reshape(1, width), bias.reshape(1, width))


def finish_kernel(res, kept, received, bias_sum, out):
    out[...] = (res[...] + (kept[...] + received[...].astype(jnp.float32) + bias_sum[...])).astype(jnp.bfloat16)


def finish(res, kept, received, bias_sum, first=0):
    tokens, width = kept.shape
    tile = 128
    row = pl.BlockSpec((tile, width), lambda n: (n, 0))
    res_row = pl.BlockSpec((tile, width), lambda n: (n + first // tile, 0))
    vec = pl.BlockSpec((1, width), lambda n: (0, 0))
    return pl.pallas_call(
        finish_kernel,
        out_shape=jax.ShapeDtypeStruct((tokens, width), jnp.bfloat16),
        grid=(tokens // tile,),
        in_specs=[res_row, row, row, vec],
        out_specs=row,
        compiler_params=pltpu.CompilerParams(vmem_limit_bytes=VMEM_LIMIT, dimension_semantics=("arbitrary",)),
        cost_estimate=pl.CostEstimate(flops=4 * tokens * width, bytes_accessed=12 * tokens * width, transcendentals=0),
    )(res, kept, received, bias_sum.reshape(1, width))


def first_kernel(res, gain, bias, h_out):
    h_out[...] = norm_block(res[...].astype(jnp.float32), gain[...], bias[...])


def first_norm(res, gain, bias):
    tokens, width = res.shape
    tile = 128
    row = pl.BlockSpec((tile, width), lambda n: (n, 0))
    vec = pl.BlockSpec((1, width), lambda n: (0, 0))
    return pl.pallas_call(
        first_kernel,
        out_shape=jax.ShapeDtypeStruct((tokens, width), jnp.bfloat16),
        grid=(tokens // tile,),
        in_specs=[row, vec, vec],
        out_specs=row,
        compiler_params=pltpu.CompilerParams(vmem_limit_bytes=VMEM_LIMIT, dimension_semantics=("arbitrary",)),
        cost_estimate=pl.CostEstimate(flops=10 * tokens * width, bytes_accessed=4 * tokens * width, transcendentals=0),
    )(res, gain.reshape(1, width), bias.reshape(1, width))


def solution(mesh):
    tp_size = mesh.shape['tp']
    act_spec = P('dp', 'tp', None)

    def swap(arr, mask):
        return lax.ppermute(arr, 'tp', [(i, i ^ mask) for i in range(tp_size)])

    SIB, XN, YN = 1, 2, 4
    HOPS = (0, SIB, YN, YN | SIB)

    def spread(shard):
        sibling = swap(shard, SIB)
        over_y = swap(shard, YN)
        diagonal = swap(over_y, SIB)
        return [shard, sibling, over_y, diagonal]

    def program(x_in, ln_gain, ln_bias, w_qkv, w_out, b_out, w_up, b_up, w_down, b_down):
        idx = lax.axis_index('tp')
        y, x, core = idx // 4, (idx // 2) % 2, idx % 2
        mine = y * 2 + core
        n_layers, width, _, heads, dim = w_qkv.shape
        batch, blk, _ = x_in.shape
        n_seq = batch // 4
        pos = jnp.stack([(((y ^ dy) * 2 + (x ^ dx)) * 2 + (core ^ dc)) * blk
                         for dx in (0, 1) for dy in (0, 1) for dc in (0, 1)]).astype(jnp.int32)

        by_group = x_in.reshape(4, n_seq, blk, width)
        parts = [[lax.dynamic_index_in_dim(by_group[:, k], mine ^ j, 0, keepdims=False) for j in range(4)]
                 for k in range(n_seq)]
        parts, w_qkv, w_up, w_down, w_out = lax.optimization_barrier((parts, w_qkv, w_up, w_down, w_out))
        residual = []
        for k in range(n_seq):
            pieces = []
            for j, mask in enumerate(HOPS):
                pieces.append(swap(parts[k][j], mask) if mask else parts[k][j])
            residual.append(jnp.concatenate(pieces, axis=0))

        b_up_all = spread(b_up)
        weights = []
        for l in range(n_layers):
            qkv_t = jnp.transpose(w_qkv[l], (1, 2, 3, 0)).reshape(3 * heads * dim, width)
            up_l, down_l, out_l = w_up[l], w_down[l], w_out[l].reshape(heads * dim, width)
            weights.append((spread(qkv_t), spread(up_l), spread(down_l),
                            jnp.concatenate(spread(out_l), axis=0)))

        h_own, finals = [], []
        for k in range(n_seq):
            h_own.append(first_norm(residual[k], ln_gain[0], ln_bias[0]))
        for l in range(n_layers):
            qkv_w, up_w, down_w, out_w = weights[l]
            bias_sum = b_out[l] + b_down[l]
            biases = [b[l] for b in b_up_all]
            for k in range(n_seq):
                h_other = swap(h_own[k], XN)
                qkv, gelu = [], []
                for h in (h_own[k], h_other):
                    qkv.append([])
                    gelu.append([])
                    for at in (0, 2):
                        qkv[-1] += qkv_pair(h, *qkv_w[at:at + 2])
                        if l == 0:
                            gelu[-1] += up(h, up_w[at:at + 2], biases[at:at + 2])
                    if l:
                        gelu[-1] += up(h, up_w, biases)
                o_own, o_oth = attention(pos, qkv[0], qkv[1], heads, dim)
                lhs_own, lhs_oth, rhs = [o_own] + gelu[0], [o_oth] + gelu[1], [out_w] + down_w
                if (l, k) == (n_layers - 1, n_seq - 1):
                    half = h_own[k].shape[0] // 2
                    ends = []
                    for first in (half, 0):
                        sent = combine(lhs_oth, rhs, jnp.bfloat16, first, half)
                        kept = combine(lhs_own, rhs, jnp.float32, first, half)
                        received = swap(sent, XN)
                        ends.append(finish(residual[k], kept, received, bias_sum, first))
                    finals.append(ends[1:] + ends[:1])
                    continue
                sent = combine(lhs_oth, rhs, jnp.bfloat16)
                kept = combine(lhs_own, rhs, jnp.float32)
                received = swap(sent, XN)
                if l + 1 < n_layers:
                    residual[k], h_own[k] = update_norm(residual[k], kept, received, bias_sum,
                                                        ln_gain[l + 1], ln_bias[l + 1])
                else:
                    finals.append([finish(residual[k], kept, received, bias_sum)])

        out = jnp.zeros((4, n_seq, blk, width), jnp.bfloat16)
        for k in range(n_seq):
            blocks = [f[at:at + blk] for f in finals[k] for at in range(0, f.shape[0], blk)]
            for j, mask in enumerate(HOPS):
                piece = blocks[j]
                piece = swap(piece, mask) if mask else piece
                out = lax.dynamic_update_slice(out, piece[None, None], (mine ^ j, k, 0, 0))
        return out.reshape(batch, blk, width)

    in_specs = (act_spec, P(), P(), P(None, None, None, 'tp', None), P(None, 'tp', None, None), P(),
                P(None, None, 'tp'), P(None, 'tp'), P(None, 'tp', None), P())
    return jax.shard_map(program, mesh=mesh, in_specs=in_specs, out_specs=act_spec, check_vma=False)
```
